32 devices in a mesh: gx: 4 (over y, x), gy: 4 (over z), gz: 2 (over core).
Axes of the slice: x: 2, y: 2, z: 4, core: 2. Of those that a mesh axis runs over, the one named last changes fastest.
Arguments:
- displacement: float32 [4, 4, 9216], P('gx', 'gy', 'gz'), may hold values from -0.1 to 0.1
- species: int32 [4, 4, 3072], P('gx', 'gy', 'gz'), may hold values from 0 to 1
- centres: int32 [4, 4, 32], P('gx', 'gy', 'gz'), may hold values from 0 to 1535, as said below
- neighbours: int32 [4, 4, 1024], P('gx', 'gy', 'gz'), may hold values from 0 to 5183, as said below
- neighbour_count: int32 [4, 4, 32], P('gx', 'gy', 'gz'), may hold values from 1 to 32, as said below
- live_centres: int32 [4, 4, 2], P('gx', 'gy', 'gz'), may hold values from 8 to 16, as said below
- w_two: float32 [12, 64], replicated, may hold values from -1.75 to 1.75
- w_lat: float32 [64, 64], replicated, may hold values from -0.75 to 0.75
- w_env: float32 [64, 64], replicated, may hold values from -0.75 to 0.75
- w_out: float32 [256, 64], replicated, may hold values from -0.375 to 0.375
- readout: float32 [64], replicated, may hold values from -0.75 to 0.75
Outputs:
- centre_energy: float32 [4, 4, 32], P('gx', 'gy', 'gz')
- forces: float32 [4, 4, 9216], P('gx', 'gy', 'gz')
The draws below stay inside these ranges and needn't reach their ends.
Inputs may be any that keep to these rules, and one draw needn't show every extreme that they name: `centres`: local atom index of an owned atom; entries may repeat. `neighbours`: extended index of an atom whose cell lies within two cells of the centre's cell in each dimension, with squared cell distance at most 4; never the centre itself. `neighbour_count`: in every domain some centre has all 32 slots live. `live_centres`: some domain has all 16 centres live; the live centres are the first ones.
All inputs are finite; a program needn't handle non-finite values.
Results may differ from the reference program's by a relative error of at most 0.0003.
Values sent between devices are 32-bit elements; how exact they have to be, the bound alone decides.
A program may use at most 64 MiB of HBM per device.

```python
import math
import jax
import jax.numpy as jnp
import numpy as np
from jax import lax

CELLS = 8
CENTRES = 16
NEIGH = 32
LATENT = 64
NBASIS = 8
SPECIES = 2
NX = 32
NY = 32
NZ = 16
N_GX = 4
N_GY = 4
N_GZ = 2


offset_rows = np.array([[0, 0, 0]] + [[a, b, c] for a in range(-2, 3) for b in range(-2, 3) for c in range(-2, 3) if 0 < a * a + b * b + c * c <= 4], np.int32)


def pair_lists(key):
    grid_x = NX // CELLS
    grid_y = NY // CELLS
    grid_z = NZ // CELLS
    extent = CELLS + 4
    base = jax.random.fold_in(key, 7)
    key_centre, key_offset, key_atom = jax.random.split(base, 3)
    centre = jax.random.randint(key_centre, (grid_x, grid_y, grid_z, CENTRES), 0, 3 * CELLS ** 3)
    atom_first = centre % 3
    cell_first = centre // 3
    loc_z = cell_first % CELLS
    loc_y = cell_first // CELLS % CELLS
    loc_x = cell_first // (CELLS * CELLS)
    choice_offset = jax.random.randint(key_offset, (grid_x, grid_y, grid_z, CENTRES, NEIGH), 0, offset_rows.shape[0])
    table = jnp.array(offset_rows)
    offsets = table[choice_offset]
    atom_second = jax.random.randint(key_atom, (grid_x, grid_y, grid_z, CENTRES, NEIGH), 0, 3)
    clash = (choice_offset == 0) & (atom_second == atom_first[..., None])
    atom_second = jnp.where(clash, (atom_first[..., None] + 1) % 3, atom_second)
    ext_x = loc_x[..., None] + 2 + offsets[..., 0]
    ext_y = loc_y[..., None] + 2 + offsets[..., 1]
    ext_z = loc_z[..., None] + 2 + offsets[..., 2]
    second = ((ext_x * extent + ext_y) * extent + ext_z) * 3 + atom_second
    return (centre.reshape(grid_x, grid_y, grid_z * CENTRES), second.reshape(grid_x, grid_y, grid_z * CENTRES * NEIGH))


def draw_centres(key, part):
    return pair_lists(key)[0].astype(jnp.int32)


def draw_neighbours(key, part):
    return pair_lists(key)[1].astype(jnp.int32)


def draw_neighbour_count(key, part):
    grid_x = NX // CELLS
    grid_y = NY // CELLS
    grid_z = NZ // CELLS
    key_level, key_count, key_pick = jax.random.split(jax.random.fold_in(key, 11), 3)
    level = jax.random.randint(key_level, (grid_x, grid_y, grid_z), 1, 5)
    ceiling = jnp.maximum(NEIGH * level // 4, 1)
    floor_count = jnp.maximum(ceiling // 2, 1)
    counts = jax.random.randint(key_count, (grid_x, grid_y, grid_z, CENTRES), floor_count[..., None], ceiling[..., None] + 1)
    pick = jax.random.randint(key_pick, (grid_x, grid_y, grid_z, 1), 0, CENTRES)
    ranks = jnp.arange(CENTRES, dtype=jnp.int32)
    counts = jnp.where(ranks == pick, NEIGH, counts)
    return counts.reshape(grid_x, grid_y, grid_z * CENTRES).astype(jnp.int32)


def draw_live_centres(key, part):
    grid_x = NX // CELLS
    grid_y = NY // CELLS
    grid_z = NZ // CELLS
    key_live, key_pick = jax.random.split(jax.random.fold_in(key, 13), 2)
    total = grid_x * grid_y * grid_z
    live = jax.random.randint(key_live, (total,), CENTRES // 2, CENTRES + 1)
    pick = jax.random.randint(key_pick, (), 0, total)
    live = jnp.where(jnp.arange(total, dtype=jnp.int32) == pick, CENTRES, live)
    return live.reshape(grid_x, grid_y, grid_z).astype(jnp.int32)


def set_ends(values, own_key, smallest, largest):
    spot = [jax.random.randint(jax.random.fold_in(own_key, axis), (), 0, length) for axis, length in enumerate(values.shape)]
    widest = values.shape.index(max(values.shape))
    neighbour = spot[:widest] + [(spot[widest] + 1) % values.shape[widest]] + spot[widest + 1:]
    return values.at[tuple(spot)].set(smallest).at[tuple(neighbour)].set(largest)


def shard_levels(key, shape, cuts, low, top_value):
    loudness, own = 1.0, jax.random.fold_in(key, 6)
    for axis_at, parts in cuts:
        draws = jnp.exp(jax.random.uniform(jax.random.fold_in(own, axis_at), (parts,), jnp.float32, low / len(cuts), top_value / len(cuts)))
        loudness = loudness * jnp.repeat(draws, shape[axis_at] // parts).reshape([-1 if axis == axis_at else 1 for axis in range(len(shape))])
    return loudness


def normal_values(stream_key, shape, spread, reach, kind=jnp.bfloat16):
    result = jax.random.normal(stream_key, shape, jnp.float32) * spread
    return jnp.minimum(jnp.maximum(result, -reach), reach).astype(kind)


def setup_inputs(seed: int = 0) -> dict:
    seeds = jax.random.split(jax.random.key(seed), 12)
    return {
        "displacement": jnp.clip(jax.random.uniform(seeds[0], (N_GX, N_GY, N_GZ * CELLS**3 * 9), jnp.float32, -0.1, 0.1) * shard_levels(seeds[0], (N_GX, N_GY, N_GZ * CELLS**3 * 9), ((0, 4), (1, 4), (2, 2)), -0.4, 0.0), -0.1, 0.1),
        "species": set_ends(jax.random.randint(seeds[1], (N_GX, N_GY, N_GZ * CELLS**3 * 3), 0, SPECIES), jax.random.fold_in(seeds[1], 1), 0, SPECIES - 1).astype(jnp.int32),
        "centres": draw_centres(jax.random.fold_in(seeds[11], 71), 0),
        "neighbours": draw_neighbours(jax.random.fold_in(seeds[11], 71), 0),
        "neighbour_count": draw_neighbour_count(jax.random.fold_in(seeds[11], 71), 0),
        "live_centres": draw_live_centres(jax.random.fold_in(seeds[11], 71), 0),
        "w_two": normal_values(seeds[6], (2 * SPECIES + NBASIS, LATENT), (2 * SPECIES + NBASIS) ** -0.5, 1.75, jnp.float32),
        "w_lat": normal_values(seeds[7], (LATENT, LATENT), LATENT ** -0.5, 0.75, jnp.float32),
        "w_env": normal_values(seeds[8], (LATENT, LATENT), LATENT ** -0.5, 0.75, jnp.float32),
        "w_out": normal_values(seeds[9], (4 * LATENT, LATENT), (4 * LATENT) ** -0.5, 0.375, jnp.float32),
        "readout": normal_values(seeds[10], (LATENT,), LATENT ** -0.5, 0.75, jnp.float32),
    }


cutoff = 6.0
cell_side = 3.1
env_scale = 0.2
site_rows = np.array([[0.25, 0.25, 0.25], [0.75, 0.75, 0.25], [0.25, 0.75, 0.75]], np.float32)

def mixing(weight, data):
    return jnp.dot(weight.T, data, precision=lax.Precision.HIGHEST, preferred_element_type=jnp.float32)

def harmonics(unit):
    ux, uy, uz = (unit[0], unit[1], unit[2])
    root3 = math.sqrt(3.0)
    root5 = math.sqrt(5.0)
    root15 = math.sqrt(15.0)
    return jnp.stack([jnp.ones_like(ux), root3 * ux, root3 * uy, root3 * uz, root15 * ux * uy, root15 * uy * uz, 0.5 * root5 * (3.0 * uz * uz - 1.0), root15 * ux * uz, 0.5 * root15 * (ux * ux - uy * uy)], 0)

def block_energy(rvec, kind_first, kind_second, live, w_two, w_lat, w_env, w_out, readout, slots):
    dist = jnp.sqrt(lax.optimization_barrier(jnp.sum(rvec * rvec, axis=0)))
    unit = rvec / dist
    ratio = dist / cutoff
    envelope = jnp.where(ratio < 1.0, 1.0 - 28.0 * ratio ** 6 + 48.0 * ratio ** 7 - 21.0 * ratio ** 8, 0.0)
    orders = jnp.arange(1, NBASIS + 1, dtype=jnp.float32)[:, None]
    basis = math.sqrt(2.0 / cutoff) * jnp.sin(orders * math.pi * dist[None, :] / cutoff) / dist[None, :] * envelope[None, :]
    kinds = jnp.arange(SPECIES, dtype=jnp.float32)[:, None]
    first_hot = (kind_first[None, :] == kinds).astype(jnp.float32)
    second_hot = (kind_second[None, :] == kinds).astype(jnp.float32)
    inputs = jnp.concatenate([first_hot, second_hot, basis], 0)
    hidden = jax.nn.silu(mixing(w_two, inputs))
    latent = jax.nn.silu(mixing(w_lat, hidden))
    weights = mixing(w_env, latent) * (envelope * live)[None, :]
    harm = harmonics(unit)
    width = latent.shape[0]
    centre_total = rvec.shape[1] // slots
    edge = (harm[:, None, :] * weights[None, :, :]).reshape(9, width, centre_total, slots)
    environ = env_scale * lax.optimization_barrier(jnp.sum(edge, axis=3))
    product = edge * environ[:, :, :, None]
    scalars = jnp.stack([product[0], lax.optimization_barrier(jnp.sum(product[1:4], axis=0)), lax.optimization_barrier(jnp.sum(product[4:9], axis=0))], 0)
    joined = jnp.concatenate([latent, scalars.reshape(3 * width, centre_total * slots)], 0)
    updated = jax.nn.silu(mixing(w_out, joined))
    pair_energy = jnp.dot(readout, updated, precision=lax.Precision.HIGHEST) * envelope * live
    return lax.optimization_barrier(jnp.sum(pair_energy.reshape(centre_total, slots), axis=1))

def to_grid(blocks, width):
    cube = blocks.reshape(N_GX, N_GY, N_GZ, CELLS, CELLS, CELLS, width)
    return jnp.transpose(cube, (0, 3, 1, 4, 2, 5, 6)).reshape(NX, NY, NZ, width)

def reference(displacement, species, centres, neighbours, neighbour_count, live_centres, w_two, w_lat, w_env, w_out, readout):
    side = CELLS
    extent = CELLS + 4
    domains = N_GX * N_GY * N_GZ
    shifts = to_grid(displacement, 9).reshape(NX, NY, NZ, 3, 3)
    kinds = to_grid(species, 3).astype(jnp.float32)
    centre_rows = centres.reshape(domains, CENTRES)
    neighbour_rows = neighbours.reshape(domains, CENTRES * NEIGH)
    count_rows = neighbour_count.reshape(domains, CENTRES)
    alive = live_centres.reshape(domains)
    sites = jnp.array(site_rows, dtype=jnp.float32)
    slot_ids = jnp.arange(NEIGH, dtype=jnp.int32)
    centre_ids = jnp.arange(CENTRES, dtype=jnp.int32)

    def one_domain(forces, index):
        dom_x = index // (N_GY * N_GZ)
        dom_y = index // N_GZ % N_GY
        dom_z = index % N_GZ
        first = jnp.repeat(centre_rows[index], NEIGH)
        atom_first = first % 3
        cell_first = first // 3
        loc_z = cell_first % side
        loc_y = cell_first // side % side
        loc_x = cell_first // (side * side)
        glob_xi = dom_x * side + loc_x
        glob_yi = dom_y * side + loc_y
        glob_zi = dom_z * side + loc_z
        second = neighbour_rows[index]
        atom_second = second % 3
        cell_second = second // 3
        ext_z = cell_second % extent - 2
        ext_y = cell_second // extent % extent - 2
        ext_x = cell_second // (extent * extent) - 2
        glob_xj = (dom_x * side + ext_x) % NX
        glob_yj = (dom_y * side + ext_y) % NY
        glob_zj = (dom_z * side + ext_z) % NZ
        place_first = jnp.stack([loc_x, loc_y, loc_z], 0).astype(jnp.float32) + sites[atom_first].T + shifts[glob_xi, glob_yi, glob_zi, atom_first].T
        place_second = jnp.stack([ext_x, ext_y, ext_z], 0).astype(jnp.float32) + sites[atom_second].T + shifts[glob_xj, glob_yj, glob_zj, atom_second].T
        rvec = (place_second - place_first) * cell_side
        kind_first = kinds[glob_xi, glob_yi, glob_zi, atom_first]
        kind_second = kinds[glob_xj, glob_yj, glob_zj, atom_second]
        live = ((slot_ids[None, :] < count_rows[index][:, None]) & (centre_ids[:, None] < alive[index])).reshape(-1).astype(jnp.float32)

        def energy_of(vectors):
            return block_energy(vectors, kind_first, kind_second, live, w_two, w_lat, w_env, w_out, readout, NEIGH)
        energy, pullback = jax.vjp(energy_of, rvec)
        grad = pullback(jnp.ones_like(energy))[0]
        index_first = ((glob_xi * NY + glob_yi) * NZ + glob_zi) * 3 + atom_first
        index_second = ((glob_xj * NY + glob_yj) * NZ + glob_zj) * 3 + atom_second
        forces = forces.at[index_second].add(-grad.T)
        forces = forces.at[index_first].add(grad.T)
        return (forces, energy)
    start = jnp.zeros((NX * NY * NZ * 3, 3), jnp.float32)
    forces, energies = lax.scan(one_domain, start, jnp.arange(domains, dtype=jnp.int32))
    grid = forces.reshape(N_GX, CELLS, N_GY, CELLS, N_GZ, CELLS, 9)
    blocks = jnp.transpose(grid, (0, 2, 4, 1, 3, 5, 6)).reshape(N_GX, N_GY, N_GZ * CELLS * CELLS * CELLS * 9)
    return (energies.reshape(N_GX, N_GY, N_GZ * CENTRES), blocks)
```

```python
import math

import jax
import jax.numpy as jnp
from jax import lax
from jax.experimental import pallas as pl
from jax.experimental.pallas import tpu as pltpu
from jax.sharding import PartitionSpec as P

CELLS = 8
NBASIS = 8
CUTOFF = 6.0
SIDE = 3.1
ENV = 0.2
LANES = 128
ZROWS = CELLS * 9
KINDS = CELLS * 3
AXES = ("gx", "gy", "gz")

NN = (((1,), (0,)), ((), ()))
NT = (((1,), (1,)), ((), ()))


def halves(x):
    hi = x.astype(jnp.bfloat16)
    lo = (x - hi.astype(jnp.float32)).astype(jnp.bfloat16)
    return hi, lo


def raw(a, b, dims):
    return lax.dot_general(a, b, dims, preferred_element_type=jnp.float32)


def mm(a, b, dims=NN):
    ah, al = a if isinstance(a, tuple) else halves(a)
    bh, bl = b if isinstance(b, tuple) else halves(b)
    return raw(ah, bh, dims) + (raw(ah, bl, dims) + raw(al, bh, dims))


def mm_exact_b(a, b, dims=NN):
    ah, al = halves(a)
    return raw(ah, b, dims) + raw(al, b, dims)


def mm_exact_a(a, b, dims=NN):
    bh, bl = halves(b)
    return raw(a, bh, dims) + raw(a, bl, dims)


def slot_plan(depth):
    plan = []
    tile = CELLS
    for dz in [0, 1] if depth == 2 else [0, 1, -1]:
        for dx in (-1, 0, 1):
            for dy in (-1, 0, 1):
                if dx == dy == dz == 0:
                    continue
                if dx == 0 and dy == 0:
                    tiles = CELLS
                elif dz == 0 and (dx == 0 or dy == 0):
                    tiles = 2
                else:
                    tiles = 1
                plan.append((dx, dy, dz, tile, tiles))
                tile += tiles
    return plan, tile


def origin(step, tiles):
    return 0 if step >= 0 else CELLS - tiles


def wave(turns):
    f = turns - jnp.floor(turns + 0.5)
    f = jnp.where(f > 0.25, 0.5 - f, jnp.where(f < -0.25, -0.5 - f, f))
    x = f * (2.0 * math.pi)
    s = x * x
    p = -1.0 / 39916800.0
    for c in (1.0 / 362880.0, -1.0 / 5040.0, 1.0 / 120.0, -1.0 / 6.0):
        p = p * s + c
    return x + x * s * p


def divided(value, by):
    return jnp.floor((value + 0.5) * (1.0 / by))


def silu_pair(x):
    s = 1.0 / (1.0 + jnp.exp(-x))
    return x * s, s * (1.0 + x * (1.0 - s))


def kernel_body(sizes, plan, disp, spec, cen, nbr, cnt, alive, w_two, w_lat, w_env, w_out,
                readout, energy, forces, table, pack, part, got, total,
                send_a, recv_a, send_b, recv_b):
    me = tuple(lax.axis_index(a) for a in AXES)

    def peer(step, sign):
        return tuple(
            lax.rem(i + (sign * d + n), n) if d else i for i, d, n in zip(me, step, sizes)
        )

    barrier = pltpu.get_barrier_semaphore()
    for slot in plan:
        pl.semaphore_signal(
            barrier, inc=1, device_id=peer(slot[:3], 1), device_id_type=pl.DeviceIdType.MESH
        )

    dline = jnp.concatenate([disp[pl.ds(k, 4, stride=9), :] for k in range(9)], axis=1)
    sline = jnp.concatenate([spec[pl.ds(k, 4, stride=3), :] for k in range(3)], axis=1)
    sline = sline.astype(jnp.float32)
    blank = jnp.zeros((4, LANES - ZROWS - KINDS), jnp.float32)
    for j in range(16):
        table[pl.ds(j, 4, stride=16), :] = jnp.concatenate(
            [
                dline[:, ZROWS * j : ZROWS * (j + 1)],
                sline[:, KINDS * j : KINDS * (j + 1)],
                blank,
            ],
            axis=1,
        )
    for t, y in enumerate((0, 1, CELLS - 2, CELLS - 1)):
        pack[pl.ds(8 * t, 8), :] = table[pl.ds(y, 8, stride=8), :]

    pl.semaphore_wait(barrier, len(plan))
    inward = []
    for at, (dx, dy, dz, tile, tiles) in enumerate(plan):
        if dx == 0 and dy != 0:
            first = 0 if dy > 0 else 4 - tiles
            source = pack.at[pl.ds(8 * first, 8 * tiles)]
        else:
            source = table.at[pl.ds(8 * origin(dx, tiles), 8 * tiles)]
        copy = pltpu.make_async_remote_copy(
            src_ref=source,
            dst_ref=table.at[pl.ds(8 * tile, 8 * tiles)],
            send_sem=send_a.at[at],
            recv_sem=recv_a.at[at],
            device_id=peer((dx, dy, dz), -1),
            device_id_type=pl.DeviceIdType.MESH,
        )
        copy.start()
        inward.append(copy)

    pairs = nbr.shape[1]
    centre_total = cen.shape[1]
    slots = pairs // centre_total
    lane = lax.broadcasted_iota(jnp.int32, (centre_total, pairs), 1)
    row = lax.broadcasted_iota(jnp.int32, (centre_total, pairs), 0)
    mine = ((lane >= row * slots) & (lane < (row + 1) * slots)).astype(jnp.float32)
    mine16 = mine.astype(jnp.bfloat16)
    lists = jnp.concatenate(
        [cen[...], cnt[...], jnp.zeros((6, centre_total), jnp.int32)], axis=0
    ).astype(jnp.float32)
    spread = mm_exact_b(lists, mine16)
    first, count = spread[0:1], spread[1:2]
    lane1 = lax.broadcasted_iota(jnp.int32, (1, pairs), 1)
    lanef = lane1.astype(jnp.float32)
    centre_id = divided(lanef, slots)
    slot_id = lanef - centre_id * slots
    live = jnp.where(
        (slot_id < count) & (lane1 < alive[0, 0] * slots), 1.0, 0.0
    ).astype(jnp.float32)

    cell_i = divided(first, 3.0)
    atom_i = first - 3.0 * cell_i
    col_i = divided(cell_i, CELLS)
    z_i = cell_i - CELLS * col_i
    x_i = divided(col_i, CELLS)
    y_i = col_i - CELLS * x_i

    second = nbr[...].astype(jnp.float32)
    ext = CELLS + 4
    cell_j = divided(second, 3.0)
    atom_j = second - 3.0 * cell_j
    col_j = divided(cell_j, ext)
    z_j = cell_j - ext * col_j - 2.0
    x_j = divided(col_j, ext)
    y_j = col_j - ext * x_j - 2.0
    x_j = x_j - 2.0

    def side(v):
        return jnp.where(v < 0.0, -1.0, jnp.where(v >= CELLS, 1.0, 0.0))

    sx, sy, sz = side(x_j), side(y_j), side(z_j)
    x_in, y_in, z_in = x_j - CELLS * sx, y_j - CELLS * sy, z_j - CELLS * sz
    if sizes[2] == 2:
        sz = jnp.abs(sz)
    code = sx * 9.0 + sy * 3.0 + sz
    across, along = x_in * CELLS + y_in, y_in * CELLS + x_in
    line = across
    for dx, dy, dz, tile, tiles in plan:
        if dx == 0 and dy != 0:
            value = along + float(8 * tile - 8 * origin(dy, tiles))
        else:
            value = across + float(8 * tile - 8 * origin(dx, tiles))
        line = jnp.where(code == float(dx * 9 + dy * 3 + dz), value, line)

    rows = table.shape[0]
    own = CELLS * CELLS

    def hot(index, length):
        ids = lax.broadcasted_iota(jnp.int32, (length, pairs), 0)
        return jnp.where(ids == index.astype(jnp.int32), 1.0, 0.0).astype(jnp.bfloat16)

    hot_j, hot_i = hot(line, rows), hot(col_i, own)
    lanes72 = lax.broadcasted_iota(jnp.int32, (ZROWS, pairs), 0)
    lanes24 = lax.broadcasted_iota(jnp.int32, (KINDS, pairs), 0)

    def site(atom):
        one, two = atom == 1.0, atom == 2.0
        return (
            jnp.where(one, 0.75, 0.25),
            jnp.where(one | two, 0.75, 0.25),
            jnp.where(two, 0.75, 0.25),
        )

    def picked(stack, place):
        at = place.astype(jnp.int32)
        body = stack[0:ZROWS]
        out = [
            jnp.sum(jnp.where(lanes72 == 3 * at + c, body, 0.0), axis=0, keepdims=True)
            for c in range(3)
        ]
        kind = jnp.sum(
            jnp.where(lanes24 == at, stack[ZROWS : ZROWS + KINDS], 0.0), axis=0, keepdims=True
        )
        return out, kind

    def fetch(block, onehot):
        hi, lo = halves(block.T)
        return raw(hi, onehot, NN) + raw(lo, onehot, NN)

    place_i, place_j = z_i * 3.0 + atom_i, z_in * 3.0 + atom_j
    shift_i, kind_i = picked(fetch(table[pl.ds(0, own), :], hot_i), place_i)
    site_i, site_j = site(atom_i), site(atom_j)
    two = w_two[...]
    two = jnp.concatenate([two[4:12], two[0:4], jnp.zeros_like(two[0:4])], axis=0)
    two_t, lat_t, env_t, out_t = two.T, w_lat[...].T, w_env[...].T, w_out[...].T

    for copy in inward:
        copy.wait()

    shift_j, kind_j = picked(fetch(table[...], hot_j), place_j)
    rx, ry, rz = [
        ((b - a) + (tb - ta) + (sb - sa)) * SIDE
        for a, b, ta, tb, sa, sb in zip(
            (x_i, y_i, z_i), (x_j, y_j, z_j), site_i, site_j, shift_i, shift_j
        )
    ]
    dist = jnp.sqrt(rx * rx + ry * ry + rz * rz)
    inv = 1.0 / dist
    ux, uy, uz = rx * inv, ry * inv, rz * inv
    ratio = dist * (1.0 / CUTOFF)
    r2 = ratio * ratio
    r5 = r2 * r2 * ratio
    inside = ratio < 1.0
    bell = jnp.where(inside, 1.0 + r5 * ratio * (-28.0 + ratio * (48.0 - 21.0 * ratio)), 0.0)
    slope = jnp.where(
        inside, r5 * (1.0 - ratio) * (1.0 - ratio) * (-168.0 / CUTOFF), 0.0
    )
    order = (lax.broadcasted_iota(jnp.int32, (NBASIS, pairs), 0) + 1).astype(jnp.float32)
    turns = order * (dist * (0.5 / CUTOFF))
    sines, cosines = wave(turns), wave(turns + 0.25)
    norm = math.sqrt(2.0 / CUTOFF)
    basis = norm * sines * (inv * bell)
    basis_d = norm * (
        cosines * order * (inv * bell * (math.pi / CUTOFF))
        + sines * (inv * (slope - bell * inv))
    )
    kinds = [1.0 - kind_i, kind_i, 1.0 - kind_j, kind_j]
    inputs = jnp.concatenate([basis] + kinds + [jnp.zeros((4, pairs), jnp.float32)], axis=0)

    hidden, hidden_d = silu_pair(mm(two_t, inputs))
    latent, latent_d = silu_pair(mm(lat_t, hidden))
    latent_h = halves(latent)
    plain = mm(env_t, latent_h)
    scale = bell * live
    weight = plain * scale
    s3, s5, s15 = math.sqrt(3.0), math.sqrt(5.0), math.sqrt(15.0)
    harm = [
        jnp.ones_like(ux),
        s3 * ux,
        s3 * uy,
        s3 * uz,
        s15 * ux * uy,
        s15 * uy * uz,
        0.5 * s5 * (3.0 * uz * uz - 1.0),
        s15 * ux * uz,
        0.5 * s15 * (ux * ux - uy * uy),
    ]
    spread_y = halves(jnp.concatenate([h * mine for h in harm], axis=0))
    weight_h = halves(weight)
    bounds = [(0, 1), (1, 4), (4, 9)]
    cuts = [slice(a * centre_total, b * centre_total) for a, b in bounds]

    def cut(pair, s):
        return pair[0][s], pair[1][s]

    environ = ENV * mm(spread_y, weight_h, NT)
    mixed = [mm(environ[s].T, cut(spread_y, s)) for s in cuts]
    width = latent.shape[0]
    joined = jnp.concatenate([latent] + [weight * a for a in mixed], axis=0)
    updated, updated_d = silu_pair(mm(out_t, joined))
    column = jnp.broadcast_to(readout[...], (8, width)).T[:, 0:1]
    score = jnp.sum(column * updated, axis=0, keepdims=True)
    pair_energy = score * scale
    energy[...] = mm_exact_b(jnp.broadcast_to(pair_energy, (8, pairs)), mine16, NT)[0:1]

    d_out = (column * scale) * updated_d
    back = mm(w_out[...], d_out)
    d_mixed = [back[width * (k + 1) : width * (k + 2)] for k in range(3)]
    d_weight = d_mixed[0] * mixed[0] + d_mixed[1] * mixed[1] + d_mixed[2] * mixed[2]
    passing = [halves(q * weight) for q in d_mixed]
    d_environ = ENV * jnp.concatenate(
        [mm(cut(spread_y, s), p, NT) for s, p in zip(cuts, passing)], axis=0
    )
    d_weight = d_weight + mm(d_environ.T, spread_y)
    d_spread = jnp.concatenate(
        [mm(environ[s], p) for s, p in zip(cuts, passing)], axis=0
    ) + mm(d_environ, weight_h)
    d_harm = [
        jnp.sum(
            d_spread[m * centre_total : (m + 1) * centre_total] * mine, axis=0, keepdims=True
        )
        for m in range(9)
    ]
    d_scale = score + jnp.sum(d_weight * plain, axis=0, keepdims=True)
    d_latent = back[0:width] + mm(w_env[...], d_weight * scale)
    d_hidden = mm(w_lat[...], d_latent * latent_d)
    d_inputs = mm(two, d_hidden * hidden_d)
    d_dist = (
        jnp.sum(d_inputs[0:NBASIS] * basis_d, axis=0, keepdims=True) + d_scale * live * slope
    )
    dux = s3 * d_harm[1] + s15 * (uy * d_harm[4] + uz * d_harm[7] + ux * d_harm[8])
    duy = s3 * d_harm[2] + s15 * (ux * d_harm[4] + uz * d_harm[5] - uy * d_harm[8])
    duz = s3 * d_harm[3] + s15 * (uy * d_harm[5] + ux * d_harm[7]) + 3.0 * s5 * uz * d_harm[6]
    radial = d_dist - (ux * dux + uy * duy + uz * duz) * inv
    grad = [d * inv + u * radial for d, u in ((dux, ux), (duy, uy), (duz, uz))]

    def placed(place, sign):
        at = 3 * place.astype(jnp.int32)
        out = jnp.zeros((ZROWS, pairs), jnp.float32)
        for c in range(3):
            out = jnp.where(lanes72 == at + c, sign * grad[c], out)
        return jnp.concatenate(
            [out, jnp.zeros((LANES - ZROWS, pairs), jnp.float32)], axis=0
        )

    part[...] = mm_exact_a(hot_j, placed(place_j, -1.0), NT)
    outward = []
    for at, (dx, dy, dz, tile, tiles) in enumerate(plan):
        copy = pltpu.make_async_remote_copy(
            src_ref=part.at[pl.ds(8 * tile, 8 * tiles)],
            dst_ref=got.at[pl.ds(8 * tile, 8 * tiles)],
            send_sem=send_b.at[at],
            recv_sem=recv_b.at[at],
            device_id=peer((dx, dy, dz), 1),
            device_id_type=pl.DeviceIdType.MESH,
        )
        copy.start()
        outward.append(copy)
    total[...] = part[pl.ds(0, own), :] + mm_exact_a(hot_i, placed(place_i, 1.0), NT)
    for copy in outward:
        copy.wait()
    for dx, dy, dz, tile, tiles in plan:
        if dx == 0 and dy != 0:
            for t in range(tiles):
                spot = pl.ds(origin(dy, tiles) + t, 8, stride=8)
                total[spot, :] = total[spot, :] + got[pl.ds(8 * (tile + t), 8), :]
        else:
            spot = pl.ds(8 * origin(dx, tiles), 8 * tiles)
            total[spot, :] = total[spot, :] + got[pl.ds(8 * tile, 8 * tiles), :]
    final = jnp.concatenate(
        [total[pl.ds(j, 4, stride=16), :][:, 0:ZROWS] for j in range(16)], axis=1
    )
    for k in range(9):
        forces[pl.ds(k, 4, stride=9), :] = final[:, LANES * k : LANES * (k + 1)]


def solution(mesh):
    sizes = tuple(mesh.shape[a] for a in AXES)
    plan, tile_total = slot_plan(sizes[2])

    def local(displacement, species, centres, neighbours, neighbour_count, live_centres,
              w_two, w_lat, w_env, w_out, readout):
        centre_total = centres.shape[2]
        atoms = displacement.shape[2]
        vmem = pl.BlockSpec(memory_space=pltpu.VMEM)
        rows = 8 * tile_total

        def body(*refs):
            kernel_body(sizes, plan, *refs)

        energy, forces = pl.pallas_call(
            body,
            out_shape=(
                jax.ShapeDtypeStruct((1, centre_total), jnp.float32),
                jax.ShapeDtypeStruct((atoms // LANES, LANES), jnp.float32),
            ),
            in_specs=[vmem] * 5
            + [pl.BlockSpec(memory_space=pltpu.SMEM)]
            + [vmem] * 5,
            out_specs=(vmem, vmem),
            scratch_shapes=[
                pltpu.VMEM((rows, LANES), jnp.float32),
                pltpu.VMEM((32, LANES), jnp.float32),
                pltpu.VMEM((rows, LANES), jnp.float32),
                pltpu.VMEM((rows, LANES), jnp.float32),
                pltpu.VMEM((CELLS * CELLS, LANES), jnp.float32),
            ]
            + [pltpu.SemaphoreType.DMA((len(plan),))] * 4,
            compiler_params=pltpu.CompilerParams(collective_id=0, has_side_effects=True),
        )(
            displacement.reshape(-1, LANES),
            species.reshape(-1, LANES),
            centres.reshape(1, -1),
            neighbours.reshape(1, -1),
            neighbour_count.reshape(1, -1),
            live_centres.reshape(1, 1),
            w_two, w_lat, w_env, w_out, readout.reshape(1, -1),
        )
        return energy.reshape(1, 1, -1), forces.reshape(1, 1, -1)

    split = P(*AXES)
    return jax.shard_map(
        local,
        mesh=mesh,
        in_specs=(split,) * 6 + (P(),) * 5,
        out_specs=(split, split),
        check_vma=False,
    )
```

```python
import math

import jax
import jax.numpy as jnp
from jax import lax
from jax.experimental import pallas as pl
from jax.experimental.pallas import tpu as pltpu
from jax.sharding import PartitionSpec as P

CELLS = 8
NBASIS = 8
CUTOFF = 6.0
SIDE = 3.1
ENV = 0.2
LANES = 128
ZROWS = CELLS * 9
KINDS = CELLS * 3
AXES = ("gx", "gy", "gz")

NN = (((1,), (0,)), ((), ()))
NT = (((1,), (1,)), ((), ()))


def halves(x):
    hi = x.astype(jnp.bfloat16)
    lo = (x - hi.astype(jnp.float32)).astype(jnp.bfloat16)
    return hi, lo


def raw(a, b, dims):
    return lax.dot_general(a, b, dims, preferred_element_type=jnp.float32)


def mm(a, b, dims=NN):
    ah, al = a if isinstance(a, tuple) else halves(a)
    bh, bl = b if isinstance(b, tuple) else halves(b)
    return raw(ah, bh, dims) + (raw(ah, bl, dims) + raw(al, bh, dims))


def mm_exact_b(a, b, dims=NN):
    ah, al = halves(a)
    return raw(ah, b, dims) + raw(al, b, dims)


def mm_exact_a(a, b, dims=NN):
    bh, bl = halves(b)
    return raw(a, bh, dims) + raw(a, bl, dims)


def slot_plan(depth):
    plan = []
    tile = CELLS
    for dz in [0, 1] if depth == 2 else [0, 1, -1]:
        for dx in (-1, 0, 1):
            for dy in (-1, 0, 1):
                if dx == dy == dz == 0:
                    continue
                if dx == 0 and dy == 0:
                    tiles = CELLS
                elif dz == 0 and (dx == 0 or dy == 0):
                    tiles = 2
                else:
                    tiles = 1
                plan.append((dx, dy, dz, tile, tiles))
                tile += tiles
    return plan, tile


def origin(step, tiles):
    return 0 if step >= 0 else CELLS - tiles


def wave(turns):
    f = turns - jnp.floor(turns + 0.5)
    f = jnp.where(f > 0.25, 0.5 - f, jnp.where(f < -0.25, -0.5 - f, f))
    x = f * (2.0 * math.pi)
    s = x * x
    p = -1.0 / 39916800.0
    for c in (1.0 / 362880.0, -1.0 / 5040.0, 1.0 / 120.0, -1.0 / 6.0):
        p = p * s + c
    return x + x * s * p


def divided(value, by):
    return jnp.floor((value + 0.5) * (1.0 / by))


def silu_pair(x):
    s = 1.0 / (1.0 + jnp.exp(-x))
    return x * s, s * (1.0 + x * (1.0 - s))


def kernel_body(sizes, plan, disp_hbm, spec_hbm, cen_hbm, nbr_hbm, cnt_hbm, alive_hbm, two_hbm,
                lat_hbm, env_hbm, out_hbm, readout_hbm, energy, forces,
                disp, spec, cen, nbr, cnt, alive, w_two, w_lat, w_env, w_out_t, readout,
                table, pack, part, got, total, send_a, recv_a, send_b, recv_b, load):
    loads = [
        pltpu.make_async_copy(src, dst, load.at[at])
        for at, (src, dst) in enumerate(
            (
                (disp_hbm, disp),
                (spec_hbm, spec),
                (cen_hbm, cen),
                (nbr_hbm, nbr),
                (cnt_hbm, cnt),
                (alive_hbm, alive),
                (two_hbm, w_two),
                (lat_hbm, w_lat),
                (env_hbm, w_env),
                (out_hbm, w_out_t),
                (readout_hbm, readout),
            )
        )
    ]
    for copy in loads:
        copy.start()
    disp, spec, cen, nbr, cnt, alive, energy, forces = (
        ref.at[0] for ref in (disp, spec, cen, nbr, cnt, alive, energy, forces)
    )
    me = tuple(lax.axis_index(a) for a in AXES)

    def peer(step, sign):
        return tuple(
            lax.rem(i + (sign * d + n), n) if d else i for i, d, n in zip(me, step, sizes)
        )

    barrier = pltpu.get_barrier_semaphore()
    for slot in plan:
        pl.semaphore_signal(
            barrier, inc=1, device_id=peer(slot[:3], 1), device_id_type=pl.DeviceIdType.MESH
        )

    for copy in loads[:2]:
        copy.wait()
    dwide, swide = 16 * ZROWS, 16 * KINDS
    dline = jnp.concatenate([disp[:, dwide * q : dwide * (q + 1)] for q in range(4)], axis=0)
    sline = jnp.concatenate([spec[:, swide * q : swide * (q + 1)] for q in range(4)], axis=0)
    sline = sline.astype(jnp.float32)
    blank = jnp.zeros((4, LANES - ZROWS - KINDS), jnp.float32)
    for j in range(16):
        table[pl.ds(j, 4, stride=16), :] = jnp.concatenate(
            [
                dline[:, ZROWS * j : ZROWS * (j + 1)],
                sline[:, KINDS * j : KINDS * (j + 1)],
                blank,
            ],
            axis=1,
        )
    for t, y in enumerate((0, 1, CELLS - 2, CELLS - 1)):
        pack[pl.ds(8 * t, 8), :] = table[pl.ds(y, 8, stride=8), :]

    pl.semaphore_wait(barrier, len(plan))
    for dx, dy, dz, tile, tiles in plan:
        if dx == 0 and dy != 0:
            first = 0 if dy > 0 else 4 - tiles
            source = pack.at[pl.ds(8 * first, 8 * tiles)]
        else:
            source = table.at[pl.ds(8 * origin(dx, tiles), 8 * tiles)]
        copy = pltpu.make_async_remote_copy(
            src_ref=source,
            dst_ref=table.at[pl.ds(8 * tile, 8 * tiles)],
            send_sem=send_a.at[0],
            recv_sem=recv_a.at[0],
            device_id=peer((dx, dy, dz), -1),
            device_id_type=pl.DeviceIdType.MESH,
        )
        copy.start()

    for copy in loads[2:]:
        copy.wait()

    pairs = nbr.shape[1]
    centre_total = cen.shape[1]
    slots = pairs // centre_total
    lane = lax.broadcasted_iota(jnp.int32, (centre_total, pairs), 1)
    row = lax.broadcasted_iota(jnp.int32, (centre_total, pairs), 0)
    mine = ((lane >= row * slots) & (lane < (row + 1) * slots)).astype(jnp.float32)
    mine16 = mine.astype(jnp.bfloat16)
    lists = jnp.concatenate(
        [cen[...], cnt[...], jnp.zeros((6, centre_total), jnp.int32)], axis=0
    ).astype(jnp.float32)
    spread = mm_exact_b(lists, mine16)
    first, count = spread[0:1], spread[1:2]
    lane1 = lax.broadcasted_iota(jnp.int32, (1, pairs), 1)
    lanef = lane1.astype(jnp.float32)
    centre_id = divided(lanef, slots)
    slot_id = lanef - centre_id * slots
    live = jnp.where(
        (slot_id < count) & (lane1 < alive[...] * slots), 1.0, 0.0
    ).astype(jnp.float32)

    cell_i = divided(first, 3.0)
    atom_i = first - 3.0 * cell_i
    col_i = divided(cell_i, CELLS)
    z_i = cell_i - CELLS * col_i
    x_i = divided(col_i, CELLS)
    y_i = col_i - CELLS * x_i

    second = nbr[...].astype(jnp.float32)
    ext = CELLS + 4
    cell_j = divided(second, 3.0)
    atom_j = second - 3.0 * cell_j
    col_j = divided(cell_j, ext)
    z_j = cell_j - ext * col_j - 2.0
    x_j = divided(col_j, ext)
    y_j = col_j - ext * x_j - 2.0
    x_j = x_j - 2.0

    def side(v):
        return jnp.where(v < 0.0, -1.0, jnp.where(v >= CELLS, 1.0, 0.0))

    sx, sy, sz = side(x_j), side(y_j), side(z_j)
    x_in, y_in, z_in = x_j - CELLS * sx, y_j - CELLS * sy, z_j - CELLS * sz
    if sizes[2] == 2:
        sz = jnp.abs(sz)
    code = sx * 9.0 + sy * 3.0 + sz
    across, along = x_in * CELLS + y_in, y_in * CELLS + x_in
    line = across
    for dx, dy, dz, tile, tiles in plan:
        if dx == 0 and dy != 0:
            value = along + float(8 * tile - 8 * origin(dy, tiles))
        else:
            value = across + float(8 * tile - 8 * origin(dx, tiles))
        line = jnp.where(code == float(dx * 9 + dy * 3 + dz), value, line)

    rows = table.shape[0]
    own = CELLS * CELLS

    def hot(index, length):
        ids = lax.broadcasted_iota(jnp.int32, (length, pairs), 0)
        return jnp.where(ids == index.astype(jnp.int32), 1.0, 0.0).astype(jnp.bfloat16)

    hot_j, hot_i = hot(line, rows), hot(col_i, own)
    lanes72 = lax.broadcasted_iota(jnp.int32, (ZROWS, pairs), 0)
    lanes24 = lax.broadcasted_iota(jnp.int32, (KINDS, pairs), 0)

    def site(atom):
        one, two = atom == 1.0, atom == 2.0
        return (
            jnp.where(one, 0.75, 0.25),
            jnp.where(one | two, 0.75, 0.25),
            jnp.where(two, 0.75, 0.25),
        )

    def picked(stack, place):
        at = place.astype(jnp.int32)
        body = stack[0:ZROWS]
        out = [
            jnp.sum(jnp.where(lanes72 == 3 * at + c, body, 0.0), axis=0, keepdims=True)
            for c in range(3)
        ]
        kind = jnp.sum(
            jnp.where(lanes24 == at, stack[ZROWS : ZROWS + KINDS], 0.0), axis=0, keepdims=True
        )
        return out, kind

    def fetch(block, onehot):
        hi, lo = halves(block.T)
        return raw(hi, onehot, NN) + raw(lo, onehot, NN)

    place_i, place_j = z_i * 3.0 + atom_i, z_in * 3.0 + atom_j
    shift_i, kind_i = picked(fetch(table[pl.ds(0, own), :], hot_i), place_i)
    site_i, site_j = site(atom_i), site(atom_j)
    two = w_two[...]
    two = jnp.concatenate([two[4:12], two[0:4], jnp.zeros_like(two[0:4])], axis=0)
    two_t, lat_t, env_t, out_t = two.T, w_lat[...].T, w_env[...].T, w_out_t[...]

    arrived = pl.ds(own, rows - own)

    def settle(ref, send, recv):
        every = pltpu.make_async_remote_copy(
            src_ref=ref.at[arrived],
            dst_ref=ref.at[arrived],
            send_sem=send.at[0],
            recv_sem=recv.at[0],
            device_id=peer(plan[0][:3], 1),
            device_id_type=pl.DeviceIdType.MESH,
        )
        every.wait()

    settle(table, send_a, recv_a)

    shift_j, kind_j = picked(fetch(table[...], hot_j), place_j)
    rx, ry, rz = [
        ((b - a) + (tb - ta) + (sb - sa)) * SIDE
        for a, b, ta, tb, sa, sb in zip(
            (x_i, y_i, z_i), (x_j, y_j, z_j), site_i, site_j, shift_i, shift_j
        )
    ]
    dist = jnp.sqrt(rx * rx + ry * ry + rz * rz)
    inv = 1.0 / dist
    ux, uy, uz = rx * inv, ry * inv, rz * inv
    ratio = dist * (1.0 / CUTOFF)
    r2 = ratio * ratio
    r5 = r2 * r2 * ratio
    inside = ratio < 1.0
    bell = jnp.where(inside, 1.0 + r5 * ratio * (-28.0 + ratio * (48.0 - 21.0 * ratio)), 0.0)
    slope = jnp.where(
        inside, r5 * (1.0 - ratio) * (1.0 - ratio) * (-168.0 / CUTOFF), 0.0
    )
    order = (lax.broadcasted_iota(jnp.int32, (NBASIS, pairs), 0) + 1).astype(jnp.float32)
    turns = order * (dist * (0.5 / CUTOFF))
    sines, cosines = wave(turns), wave(turns + 0.25)
    norm = math.sqrt(2.0 / CUTOFF)
    basis = norm * sines * (inv * bell)
    basis_d = norm * (
        cosines * order * (inv * bell * (math.pi / CUTOFF))
        + sines * (inv * (slope - bell * inv))
    )
    kinds = [1.0 - kind_i, kind_i, 1.0 - kind_j, kind_j]
    inputs = jnp.concatenate([basis] + kinds + [jnp.zeros((4, pairs), jnp.float32)], axis=0)

    hidden, hidden_d = silu_pair(mm(two_t, inputs))
    latent, latent_d = silu_pair(mm(lat_t, hidden))
    latent_h = halves(latent)
    plain = mm(env_t, latent_h)
    scale = bell * live
    weight = plain * scale
    s3, s5, s15 = math.sqrt(3.0), math.sqrt(5.0), math.sqrt(15.0)
    harm = [
        jnp.ones_like(ux),
        s3 * ux,
        s3 * uy,
        s3 * uz,
        s15 * ux * uy,
        s15 * uy * uz,
        0.5 * s5 * (3.0 * uz * uz - 1.0),
        s15 * ux * uz,
        0.5 * s15 * (ux * ux - uy * uy),
    ]
    spread_y = halves(jnp.concatenate([h * mine for h in harm], axis=0))
    weight_h = halves(weight)
    bounds = [(0, 1), (1, 4), (4, 9)]
    cuts = [slice(a * centre_total, b * centre_total) for a, b in bounds]

    def cut(pair, s):
        return pair[0][s], pair[1][s]

    environ = ENV * mm(spread_y, weight_h, NT)
    mixed = [mm(environ[s].T, cut(spread_y, s)) for s in cuts]
    width = latent.shape[0]
    joined = jnp.concatenate([latent] + [weight * a for a in mixed], axis=0)
    updated, updated_d = silu_pair(mm(out_t, joined))
    column = jnp.broadcast_to(readout[...], (8, width)).T[:, 0:1]
    score = jnp.sum(column * updated, axis=0, keepdims=True)
    pair_energy = score * scale
    energy[...] = mm_exact_b(jnp.broadcast_to(pair_energy, (8, pairs)), mine16, NT)[0:1]

    d_out = (column * scale) * updated_d
    back = mm(out_t.T, d_out)
    d_mixed = [back[width * (k + 1) : width * (k + 2)] for k in range(3)]
    d_weight = d_mixed[0] * mixed[0] + d_mixed[1] * mixed[1] + d_mixed[2] * mixed[2]
    passing = [halves(q * weight) for q in d_mixed]
    d_environ = ENV * jnp.concatenate(
        [mm(cut(spread_y, s), p, NT) for s, p in zip(cuts, passing)], axis=0
    )
    d_weight = d_weight + mm(d_environ.T, spread_y)
    d_spread = jnp.concatenate(
        [mm(environ[s], p) for s, p in zip(cuts, passing)], axis=0
    ) + mm(d_environ, weight_h)
    d_harm = [
        jnp.sum(
            d_spread[m * centre_total : (m + 1) * centre_total] * mine, axis=0, keepdims=True
        )
        for m in range(9)
    ]
    d_scale = score + jnp.sum(d_weight * plain, axis=0, keepdims=True)
    d_latent = back[0:width] + mm(w_env[...], d_weight * scale)
    d_hidden = mm(w_lat[...], d_latent * latent_d)
    d_inputs = mm(two, d_hidden * hidden_d)
    d_dist = (
        jnp.sum(d_inputs[0:NBASIS] * basis_d, axis=0, keepdims=True) + d_scale * live * slope
    )
    dux = s3 * d_harm[1] + s15 * (uy * d_harm[4] + uz * d_harm[7] + ux * d_harm[8])
    duy = s3 * d_harm[2] + s15 * (ux * d_harm[4] + uz * d_harm[5] - uy * d_harm[8])
    duz = s3 * d_harm[3] + s15 * (uy * d_harm[5] + ux * d_harm[7]) + 3.0 * s5 * uz * d_harm[6]
    radial = d_dist - (ux * dux + uy * duy + uz * duz) * inv
    grad = [d * inv + u * radial for d, u in ((dux, ux), (duy, uy), (duz, uz))]

    def placed(place, sign):
        at = 3 * place.astype(jnp.int32)
        out = jnp.zeros((ZROWS, pairs), jnp.float32)
        for c in range(3):
            out = jnp.where(lanes72 == at + c, sign * grad[c], out)
        return jnp.concatenate(
            [out, jnp.zeros((LANES - ZROWS, pairs), jnp.float32)], axis=0
        )

    part[...] = mm_exact_a(hot_j, placed(place_j, -1.0), NT)
    for dx, dy, dz, tile, tiles in plan:
        copy = pltpu.make_async_remote_copy(
            src_ref=part.at[pl.ds(8 * tile, 8 * tiles)],
            dst_ref=got.at[pl.ds(8 * tile, 8 * tiles)],
            send_sem=send_b.at[0],
            recv_sem=recv_b.at[0],
            device_id=peer((dx, dy, dz), 1),
            device_id_type=pl.DeviceIdType.MESH,
        )
        copy.start()
    total[...] = part[pl.ds(0, own), :] + mm_exact_a(hot_i, placed(place_i, 1.0), NT)
    settle(got, send_b, recv_b)
    for dx, dy, dz, tile, tiles in plan:
        if dx == 0 and dy != 0:
            for t in range(tiles):
                spot = pl.ds(origin(dy, tiles) + t, 8, stride=8)
                total[spot, :] = total[spot, :] + got[pl.ds(8 * (tile + t), 8), :]
        else:
            spot = pl.ds(8 * origin(dx, tiles), 8 * tiles)
            total[spot, :] = total[spot, :] + got[pl.ds(8 * tile, 8 * tiles), :]
    final = jnp.concatenate(
        [total[pl.ds(j, 4, stride=16), :][:, 0:ZROWS] for j in range(16)], axis=1
    )
    for q in range(4):
        forces[:, dwide * q : dwide * (q + 1)] = final[q : q + 1, :]


def solution(mesh):
    sizes = tuple(mesh.shape[a] for a in AXES)
    plan, tile_total = slot_plan(sizes[2])

    def local(displacement, species, centres, neighbours, neighbour_count, live_centres,
              w_two, w_lat, w_env, w_out, readout):
        centre_total = centres.shape[2]
        atoms = displacement.shape[2]
        vmem = pl.BlockSpec(memory_space=pltpu.VMEM)
        rows = 8 * tile_total
        args = [
            displacement, species, centres, neighbours, neighbour_count, live_centres,
            w_two, w_lat, w_env, w_out.T, readout.reshape(1, -1),
        ]

        def body(*refs):
            kernel_body(sizes, plan, *refs)

        return pl.pallas_call(
            body,
            out_shape=(
                jax.ShapeDtypeStruct(centres.shape, jnp.float32),
                jax.ShapeDtypeStruct(displacement.shape, jnp.float32),
            ),
            in_specs=[pl.BlockSpec(memory_space=pltpu.HBM)] * len(args),
            out_specs=(vmem, vmem),
            scratch_shapes=[pltpu.VMEM(x.shape, x.dtype) for x in args]
            + [
                pltpu.VMEM((rows, LANES), jnp.float32),
                pltpu.VMEM((32, LANES), jnp.float32),
                pltpu.VMEM((rows, LANES), jnp.float32),
                pltpu.VMEM((rows, LANES), jnp.float32),
                pltpu.VMEM((CELLS * CELLS, LANES), jnp.float32),
            ]
            + [pltpu.SemaphoreType.DMA((1,))] * 4
            + [pltpu.SemaphoreType.DMA((len(args),))],
            compiler_params=pltpu.CompilerParams(collective_id=0, has_side_effects=True),
        )(*args)

    split = P(*AXES)
    return jax.shard_map(
        local,
        mesh=mesh,
        in_specs=(split,) * 6 + (P(),) * 5,
        out_specs=(split, split),
        check_vma=False,
    )
```

```python
import math

import jax
import jax.numpy as jnp
from jax import lax
from jax.experimental import pallas as pl
from jax.experimental.pallas import tpu as pltpu
from jax.sharding import PartitionSpec as P

CELLS = 8
NBASIS = 8
CUTOFF = 6.0
SIDE = 3.1
ENV = 0.2
LANES = 128
ZROWS = CELLS * 9
KINDS = CELLS * 3
AXES = ("gx", "gy", "gz")

NN = (((1,), (0,)), ((), ()))
NT = (((1,), (1,)), ((), ()))


def halves(x):
    hi = x.astype(jnp.bfloat16)
    lo = (x - hi.astype(jnp.float32)).astype(jnp.bfloat16)
    return hi, lo


def raw(a, b, dims):
    return lax.dot_general(a, b, dims, preferred_element_type=jnp.float32)


def mm(a, b, dims=NN):
    ah, al = a if isinstance(a, tuple) else halves(a)
    bh, bl = b if isinstance(b, tuple) else halves(b)
    if dims is NT:
        m, n = ah.shape[0], bh.shape[0]
        both = raw(jnp.concatenate([ah, al], axis=0), jnp.concatenate([bh, bl], axis=0), NT)
        return both[:m, :n] + (both[:m, n:] + both[m:, :n])
    if ah.shape[1] > 2 * LANES - 1:
        return raw(ah, bh, dims) + (raw(ah, bl, dims) + raw(al, bh, dims))
    return raw(
        jnp.concatenate([ah, ah, al], axis=1), jnp.concatenate([bh, bl, bh], axis=0), NN
    )


def mm_exact_b(a, b, dims=NN):
    ah, al = halves(a)
    return raw(ah, b, dims) + raw(al, b, dims)


def mm_exact_a(a, b):
    n = b.shape[0]
    both = raw(a, jnp.concatenate(halves(b), axis=0), NT)
    return both[:, :n] + both[:, n:]


def slot_plan(depth):
    plan = []
    tile = CELLS
    for dz in [0, 1] if depth == 2 else [0, 1, -1]:
        for dx in (-1, 0, 1):
            for dy in (-1, 0, 1):
                if dx == dy == dz == 0:
                    continue
                if dx == 0 and dy == 0:
                    tiles = CELLS
                elif dz == 0 and (dx == 0 or dy == 0):
                    tiles = 2
                else:
                    tiles = 1
                plan.append((dx, dy, dz, tile, tiles))
                tile += tiles
    return plan, tile


def origin(step, tiles):
    return 0 if step >= 0 else CELLS - tiles


def wave(turns):
    f = turns - jnp.floor(turns + 0.5)
    f = jnp.where(f > 0.25, 0.5 - f, jnp.where(f < -0.25, -0.5 - f, f))
    x = f * (2.0 * math.pi)
    s = x * x
    p = -1.0 / 39916800.0
    for c in (1.0 / 362880.0, -1.0 / 5040.0, 1.0 / 120.0, -1.0 / 6.0):
        p = p * s + c
    return x + x * s * p


def divided(value, by):
    return jnp.floor((value + 0.5) * (1.0 / by))


def silu_pair(x):
    s = 1.0 / (1.0 + jnp.exp(-x))
    return x * s, s * (1.0 + x * (1.0 - s))


def kernel_body(sizes, plan, disp_hbm, spec_hbm, cen_hbm, nbr_hbm, cnt_hbm, alive_hbm, two_hbm,
                lat_hbm, env_hbm, out_hbm, readout_hbm, result,
                disp, spec, cen, nbr, cnt, alive, w_two, w_lat, w_env, w_out_t, readout,
                table, pack, part, got, send_a, recv_a, send_b, recv_b, load):
    loads = [
        pltpu.make_async_copy(src, dst, load.at[at])
        for at, (src, dst) in enumerate(
            (
                (disp_hbm, disp),
                (spec_hbm, spec),
                (cen_hbm, cen),
                (nbr_hbm, nbr),
                (cnt_hbm, cnt),
                (alive_hbm, alive),
                (two_hbm, w_two),
                (lat_hbm, w_lat),
                (env_hbm, w_env),
                (out_hbm, w_out_t),
                (readout_hbm, readout),
            )
        )
    ]
    for copy in loads:
        copy.start()
    disp, spec, cen, nbr, cnt, alive = (
        ref.at[0] for ref in (disp, spec, cen, nbr, cnt, alive)
    )
    total = result.at[pl.ds(0, CELLS * CELLS)]
    me = tuple(lax.axis_index(a) for a in AXES)

    def peer(step, sign):
        return tuple(
            lax.rem(i + (sign * d + n), n) if d else i for i, d, n in zip(me, step, sizes)
        )

    barrier = pltpu.get_barrier_semaphore()
    for slot in plan:
        pl.semaphore_signal(
            barrier, inc=1, device_id=peer(slot[:3], 1), device_id_type=pl.DeviceIdType.MESH
        )

    for copy in loads[:2]:
        copy.wait()
    dwide, swide = 16 * ZROWS, 16 * KINDS
    dline = jnp.concatenate([disp[:, dwide * q : dwide * (q + 1)] for q in range(4)], axis=0)
    sline = jnp.concatenate([spec[:, swide * q : swide * (q + 1)] for q in range(4)], axis=0)
    sline = sline.astype(jnp.float32)
    blank = jnp.zeros((4, LANES - ZROWS - KINDS), jnp.float32)
    for j in range(16):
        table[pl.ds(j, 4, stride=16), :] = jnp.concatenate(
            [
                dline[:, ZROWS * j : ZROWS * (j + 1)],
                sline[:, KINDS * j : KINDS * (j + 1)],
                blank,
            ],
            axis=1,
        )
    for t, y in enumerate((0, 1, CELLS - 2, CELLS - 1)):
        pack[pl.ds(8 * t, 8), :] = table[pl.ds(y, 8, stride=8), :]

    pl.semaphore_wait(barrier, len(plan))
    for dx, dy, dz, tile, tiles in plan:
        if dx == 0 and dy != 0:
            first = 0 if dy > 0 else 4 - tiles
            source = pack.at[pl.ds(8 * first, 8 * tiles)]
        else:
            source = table.at[pl.ds(8 * origin(dx, tiles), 8 * tiles)]
        copy = pltpu.make_async_remote_copy(
            src_ref=source,
            dst_ref=table.at[pl.ds(8 * tile, 8 * tiles)],
            send_sem=send_a.at[0],
            recv_sem=recv_a.at[0],
            device_id=peer((dx, dy, dz), -1),
            device_id_type=pl.DeviceIdType.MESH,
        )
        copy.start()

    for copy in loads[2:]:
        copy.wait()

    pairs = nbr.shape[1]
    centre_total = cen.shape[1]
    slots = pairs // centre_total
    lane = lax.broadcasted_iota(jnp.int32, (centre_total, pairs), 1)
    row = lax.broadcasted_iota(jnp.int32, (centre_total, pairs), 0)
    mine = ((lane >= row * slots) & (lane < (row + 1) * slots)).astype(jnp.float32)
    mine16 = mine.astype(jnp.bfloat16)
    lists = jnp.concatenate(
        [cen[...], cnt[...], jnp.zeros((6, centre_total), jnp.int32)], axis=0
    ).astype(jnp.float32)
    spread = mm_exact_b(lists, mine16)
    first, count = spread[0:1], spread[1:2]
    lane1 = lax.broadcasted_iota(jnp.int32, (1, pairs), 1)
    lanef = lane1.astype(jnp.float32)
    centre_id = divided(lanef, slots)
    slot_id = lanef - centre_id * slots
    live = jnp.where(
        (slot_id < count) & (lane1 < alive[...] * slots), 1.0, 0.0
    ).astype(jnp.float32)

    cell_i = divided(first, 3.0)
    atom_i = first - 3.0 * cell_i
    col_i = divided(cell_i, CELLS)
    z_i = cell_i - CELLS * col_i
    x_i = divided(col_i, CELLS)
    y_i = col_i - CELLS * x_i

    second = nbr[...].astype(jnp.float32)
    ext = CELLS + 4
    cell_j = divided(second, 3.0)
    atom_j = second - 3.0 * cell_j
    col_j = divided(cell_j, ext)
    z_j = cell_j - ext * col_j - 2.0
    x_j = divided(col_j, ext)
    y_j = col_j - ext * x_j - 2.0
    x_j = x_j - 2.0

    def side(v):
        return jnp.where(v < 0.0, -1.0, jnp.where(v >= CELLS, 1.0, 0.0))

    sx, sy, sz = side(x_j), side(y_j), side(z_j)
    x_in, y_in, z_in = x_j - CELLS * sx, y_j - CELLS * sy, z_j - CELLS * sz
    if sizes[2] == 2:
        sz = jnp.abs(sz)
    code = sx * 9.0 + sy * 3.0 + sz
    across, along = x_in * CELLS + y_in, y_in * CELLS + x_in
    line = across
    for dx, dy, dz, tile, tiles in plan:
        if dx == 0 and dy != 0:
            value = along + float(8 * tile - 8 * origin(dy, tiles))
        else:
            value = across + float(8 * tile - 8 * origin(dx, tiles))
        line = jnp.where(code == float(dx * 9 + dy * 3 + dz), value, line)

    rows = table.shape[0]
    own = CELLS * CELLS

    def hot(index, length):
        ids = lax.broadcasted_iota(jnp.int32, (length, pairs), 0)
        return jnp.where(ids == index.astype(jnp.int32), 1.0, 0.0).astype(jnp.bfloat16)

    hot_j, hot_i = hot(line, rows), hot(col_i, own)
    lanes72 = lax.broadcasted_iota(jnp.int32, (ZROWS, pairs), 0)
    lanes24 = lax.broadcasted_iota(jnp.int32, (KINDS, pairs), 0)

    def site(atom):
        one, two = atom == 1.0, atom == 2.0
        return (
            jnp.where(one, 0.75, 0.25),
            jnp.where(one | two, 0.75, 0.25),
            jnp.where(two, 0.75, 0.25),
        )

    def picked(stack, place):
        at = place.astype(jnp.int32)
        body = stack[0:ZROWS]
        out = [
            jnp.sum(jnp.where(lanes72 == 3 * at + c, body, 0.0), axis=0, keepdims=True)
            for c in range(3)
        ]
        kind = jnp.sum(
            jnp.where(lanes24 == at, stack[ZROWS : ZROWS + KINDS], 0.0), axis=0, keepdims=True
        )
        return out, kind

    def fetch(block, onehot):
        both = raw(jnp.concatenate(halves(block.T), axis=0), onehot, NN)
        return both[:LANES] + both[LANES:]

    place_i, place_j = z_i * 3.0 + atom_i, z_in * 3.0 + atom_j
    shift_i, kind_i = picked(fetch(table[pl.ds(0, own), :], hot_i), place_i)
    site_i, site_j = site(atom_i), site(atom_j)
    two = w_two[...]
    two = jnp.concatenate([two[4:12], two[0:4], jnp.zeros_like(two[0:4])], axis=0)
    two_t, lat_t, env_t, out_t = two.T, w_lat[...].T, w_env[...].T, w_out_t[...]

    arrived = pl.ds(own, rows - own)

    def settle(ref, send, recv):
        every = pltpu.make_async_remote_copy(
            src_ref=ref.at[arrived],
            dst_ref=ref.at[arrived],
            send_sem=send.at[0],
            recv_sem=recv.at[0],
            device_id=peer(plan[0][:3], 1),
            device_id_type=pl.DeviceIdType.MESH,
        )
        every.wait()

    settle(table, send_a, recv_a)

    shift_j, kind_j = picked(fetch(table[...], hot_j), place_j)
    rx, ry, rz = [
        ((b - a) + (tb - ta) + (sb - sa)) * SIDE
        for a, b, ta, tb, sa, sb in zip(
            (x_i, y_i, z_i), (x_j, y_j, z_j), site_i, site_j, shift_i, shift_j
        )
    ]
    dist = jnp.sqrt(rx * rx + ry * ry + rz * rz)
    inv = 1.0 / dist
    ux, uy, uz = rx * inv, ry * inv, rz * inv
    ratio = dist * (1.0 / CUTOFF)
    r2 = ratio * ratio
    r5 = r2 * r2 * ratio
    inside = ratio < 1.0
    bell = jnp.where(inside, 1.0 + r5 * ratio * (-28.0 + ratio * (48.0 - 21.0 * ratio)), 0.0)
    slope = jnp.where(
        inside, r5 * (1.0 - ratio) * (1.0 - ratio) * (-168.0 / CUTOFF), 0.0
    )
    order = (lax.broadcasted_iota(jnp.int32, (NBASIS, pairs), 0) + 1).astype(jnp.float32)
    turns = order * (dist * (0.5 / CUTOFF))
    sines, cosines = wave(turns), wave(turns + 0.25)
    norm = math.sqrt(2.0 / CUTOFF)
    basis = norm * sines * (inv * bell)
    basis_d = norm * (
        cosines * order * (inv * bell * (math.pi / CUTOFF))
        + sines * (inv * (slope - bell * inv))
    )
    kinds = [1.0 - kind_i, kind_i, 1.0 - kind_j, kind_j]
    inputs = jnp.concatenate([basis] + kinds + [jnp.zeros((4, pairs), jnp.float32)], axis=0)

    hidden, hidden_d = silu_pair(mm(two_t, inputs))
    latent, latent_d = silu_pair(mm(lat_t, hidden))
    latent_h = halves(latent)
    plain = mm(env_t, latent_h)
    scale = bell * live
    weight = plain * scale
    s3, s5, s15 = math.sqrt(3.0), math.sqrt(5.0), math.sqrt(15.0)
    harm = [
        jnp.ones_like(ux),
        s3 * ux,
        s3 * uy,
        s3 * uz,
        s15 * ux * uy,
        s15 * uy * uz,
        0.5 * s5 * (3.0 * uz * uz - 1.0),
        s15 * ux * uz,
        0.5 * s15 * (ux * ux - uy * uy),
    ]
    spread_y = halves(jnp.concatenate([h * mine for h in harm], axis=0))
    weight_h = halves(weight)
    bounds = [(0, 1), (1, 4), (4, 9)]
    cuts = [slice(a * centre_total, b * centre_total) for a, b in bounds]

    def cut(pair, s):
        return pair[0][s], pair[1][s]

    environ = ENV * mm(spread_y, weight_h, NT)
    mixed = [mm(environ[s].T, cut(spread_y, s)) for s in cuts]
    width = latent.shape[0]
    joined = jnp.concatenate([latent] + [weight * a for a in mixed], axis=0)
    updated, updated_d = silu_pair(mm(out_t, joined))
    column = jnp.broadcast_to(readout[...], (8, width)).T[:, 0:1]
    score = jnp.sum(column * updated, axis=0, keepdims=True)
    pair_energy = score * scale
    energies = mm_exact_b(jnp.broadcast_to(pair_energy, (8, pairs)), mine16, NT)
    result[pl.ds(CELLS * CELLS, 8), 0:centre_total] = energies

    d_out = (column * scale) * updated_d
    back = mm(out_t.T, d_out)
    d_mixed = [back[width * (k + 1) : width * (k + 2)] for k in range(3)]
    d_weight = d_mixed[0] * mixed[0] + d_mixed[1] * mixed[1] + d_mixed[2] * mixed[2]
    passing = [halves(q * weight) for q in d_mixed]
    d_environ = ENV * jnp.concatenate(
        [mm(cut(spread_y, s), p, NT) for s, p in zip(cuts, passing)], axis=0
    )
    d_weight = d_weight + mm(d_environ.T, spread_y)
    d_spread = jnp.concatenate(
        [mm(environ[s], p) for s, p in zip(cuts, passing)], axis=0
    ) + mm(d_environ, weight_h)
    d_harm = [
        jnp.sum(
            d_spread[m * centre_total : (m + 1) * centre_total] * mine, axis=0, keepdims=True
        )
        for m in range(9)
    ]
    d_scale = score + jnp.sum(d_weight * plain, axis=0, keepdims=True)
    d_latent = back[0:width] + mm(w_env[...], d_weight * scale)
    d_hidden = mm(w_lat[...], d_latent * latent_d)
    d_inputs = mm(two, d_hidden * hidden_d)
    d_dist = (
        jnp.sum(d_inputs[0:NBASIS] * basis_d, axis=0, keepdims=True) + d_scale * live * slope
    )
    dux = s3 * d_harm[1] + s15 * (uy * d_harm[4] + uz * d_harm[7] + ux * d_harm[8])
    duy = s3 * d_harm[2] + s15 * (ux * d_harm[4] + uz * d_harm[5] - uy * d_harm[8])
    duz = s3 * d_harm[3] + s15 * (uy * d_harm[5] + ux * d_harm[7]) + 3.0 * s5 * uz * d_harm[6]
    radial = d_dist - (ux * dux + uy * duy + uz * duz) * inv
    grad = [d * inv + u * radial for d, u in ((dux, ux), (duy, uy), (duz, uz))]

    def placed(place, sign):
        at = 3 * place.astype(jnp.int32)
        out = jnp.zeros((ZROWS, pairs), jnp.float32)
        for c in range(3):
            out = jnp.where(lanes72 == at + c, sign * grad[c], out)
        return jnp.concatenate(
            [out, jnp.zeros((LANES - ZROWS, pairs), jnp.float32)], axis=0
        )

    part[...] = mm_exact_a(hot_j, placed(place_j, -1.0))
    for dx, dy, dz, tile, tiles in plan:
        copy = pltpu.make_async_remote_copy(
            src_ref=part.at[pl.ds(8 * tile, 8 * tiles)],
            dst_ref=got.at[pl.ds(8 * tile, 8 * tiles)],
            send_sem=send_b.at[0],
            recv_sem=recv_b.at[0],
            device_id=peer((dx, dy, dz), 1),
            device_id_type=pl.DeviceIdType.MESH,
        )
        copy.start()
    total[...] = part[pl.ds(0, own), :] + mm_exact_a(hot_i, placed(place_i, 1.0))
    settle(got, send_b, recv_b)
    for dx, dy, dz, tile, tiles in plan:
        if dx == 0 and dy != 0:
            for t in range(tiles):
                spot = pl.ds(origin(dy, tiles) + t, 8, stride=8)
                total[spot, :] = total[spot, :] + got[pl.ds(8 * (tile + t), 8), :]
        else:
            spot = pl.ds(8 * origin(dx, tiles), 8 * tiles)
            total[spot, :] = total[spot, :] + got[pl.ds(8 * tile, 8 * tiles), :]


def unpack_body(result, energy, forces):
    energy[0] = result[pl.ds(CELLS * CELLS, 1), 0 : energy.shape[2]]
    final = jnp.concatenate(
        [result[pl.ds(j, 4, stride=16), :][:, 0:ZROWS] for j in range(16)], axis=1
    )
    wide = 16 * ZROWS
    for q in range(4):
        forces[0, :, wide * q : wide * (q + 1)] = final[q : q + 1, :]


def solution(mesh):
    sizes = tuple(mesh.shape[a] for a in AXES)
    plan, tile_total = slot_plan(sizes[2])

    def local(displacement, species, centres, neighbours, neighbour_count, live_centres,
              w_two, w_lat, w_env, w_out, readout):
        centre_total = centres.shape[2]
        atoms = displacement.shape[2]
        vmem = pl.BlockSpec(memory_space=pltpu.VMEM)
        rows = 8 * tile_total
        args = [
            displacement, species, centres, neighbours, neighbour_count, live_centres,
            w_two, w_lat, w_env, w_out.T, readout.reshape(1, -1),
        ]

        def body(*refs):
            kernel_body(sizes, plan, *refs)

        result = pl.pallas_call(
            body,
            out_shape=jax.ShapeDtypeStruct((CELLS * CELLS + 8, LANES), jnp.float32),
            in_specs=[pl.BlockSpec(memory_space=pltpu.HBM)] * len(args),
            out_specs=vmem,
            scratch_shapes=[pltpu.VMEM(x.shape, x.dtype) for x in args]
            + [
                pltpu.VMEM((rows, LANES), jnp.float32),
                pltpu.VMEM((32, LANES), jnp.float32),
                pltpu.VMEM((rows, LANES), jnp.float32),
                pltpu.VMEM((rows, LANES), jnp.float32),
            ]
            + [pltpu.SemaphoreType.DMA((1,))] * 4
            + [pltpu.SemaphoreType.DMA((len(args),))],
            compiler_params=pltpu.CompilerParams(collective_id=0, has_side_effects=True),
        )(*args)
        return pl.pallas_call(
            unpack_body,
            out_shape=(
                jax.ShapeDtypeStruct(centres.shape, jnp.float32),
                jax.ShapeDtypeStruct(displacement.shape, jnp.float32),
            ),
            in_specs=[vmem],
            out_specs=(vmem, vmem),
        )(result)

    split = P(*AXES)
    return jax.shard_map(
        local,
        mesh=mesh,
        in_specs=(split,) * 6 + (P(),) * 5,
        out_specs=(split, split),
        check_vma=False,
    )
```
